32 devices in a mesh: rep: 4 (over x, y), dp: 8 (over z, core).
Axes of the slice: x: 2, y: 2, z: 4, core: 2. Of those that a mesh axis runs over, the one named last changes fastest.
Arguments:
- x: bfloat16 [32, 4096, 768], P(('rep', 'dp')), parts along dimension 0
- dy: bfloat16 [32, 4096, 768], P(('rep', 'dp')), parts along dimension 0
- w_gate: bfloat16 [2, 768, 2304], P(None, 'dp')
- w_up: bfloat16 [2, 768, 2304], P(None, 'dp')
- w_down: bfloat16 [2, 2304, 768], P(None, 'dp')
- m_w_gate: float32 [2, 768, 2304], P(None, 'dp')
- m_w_up: float32 [2, 768, 2304], P(None, 'dp')
- m_w_down: float32 [2, 2304, 768], P(None, 'dp')
- v_w_gate: float32 [2, 768, 2304], P(None, 'dp')
- v_w_up: float32 [2, 768, 2304], P(None, 'dp')
- v_w_down: float32 [2, 2304, 768], P(None, 'dp')
Outputs:
- output 1: bfloat16 [8, 768, 2304], P('rep', 'dp'), parts along dimension 0
- output 2: bfloat16 [8, 768, 2304], P('rep', 'dp'), parts along dimension 0
- output 3: bfloat16 [8, 2304, 768], P('rep', 'dp'), parts along dimension 0
- output 4: float32 [8, 768, 2304], P('rep', 'dp'), parts along dimension 0
- output 5: float32 [8, 768, 2304], P('rep', 'dp'), parts along dimension 0
- output 6: float32 [8, 2304, 768], P('rep', 'dp'), parts along dimension 0
- output 7: float32 [8, 768, 2304], P('rep', 'dp'), parts along dimension 0
- output 8: float32 [8, 768, 2304], P('rep', 'dp'), parts along dimension 0
- output 9: float32 [8, 2304, 768], P('rep', 'dp'), parts along dimension 0
There are 4 independent parts. The reference program is written for one: setup_inputs(seed, part) draws one part's arguments, and reference() takes and returns one part's arrays. A program takes and returns all parts, laid end to end along the dimension named above; an argument that names none is the same for every part.
All inputs are finite; a program needn't handle non-finite values.
Results may differ from the reference program's by a relative error of at most 0.022.
Values are sent between devices in bfloat16 or wider.
A program may use at most 2 GiB of HBM per device.

```python
import jax
import jax.numpy as jnp
from jax import lax

SEQUENCES = 8
TOKENS = 4096
D = 768
FF = 2304
LAYERS = 2
NAMES = ("w_gate", "w_up", "w_down")
SHAPES = {"w_gate": (LAYERS, D, FF), "w_up": (LAYERS, D, FF), "w_down": (LAYERS, FF, D)}


def bump(key, n, height):
    away = (jnp.arange(n, dtype=jnp.int32) - jax.random.randint(key, (), 0, n, jnp.int32)) % n
    return jnp.where(away < n // 8, height, 1.0)


def together(key, own, strength):
    shared = jax.random.normal(key, own.shape[1:], jnp.float32)
    return (own + strength * shared) * lax.rsqrt(1 + strength * strength)


def setup_inputs(seed: int = 0, part: int = 0) -> dict:
    kx, kdy, ka, kb, kz, kf, kh, kl, *keys = jax.random.split(jax.random.key(seed), 8 + 3 * len(NAMES))
    kx, kdy, ka, kb = (jax.random.fold_in(k, part) for k in (kx, kdy, ka, kb))
    kw, km, kv = (keys[i::3] for i in range(3))
    shape = (SEQUENCES, TOKENS, D)
    much_x, much_dy = jax.random.uniform(kz, (2,), jnp.float32, 0.0, 1.0)
    loud = 2.0 ** jax.random.uniform(jax.random.fold_in(kz, 1), (), jnp.float32, -1.0, 2.0)
    layers = 2.0 ** jax.random.uniform(kl, (LAYERS, 1, 1), jnp.float32, -1.0, 1.0)
    x = together(ka, jax.random.normal(kx, shape, jnp.float32), much_x) * bump(kf, D, 4.0)
    dy = together(kb, jax.random.normal(kdy, shape, jnp.float32), much_dy)
    drawn = {"x": x.astype(jnp.bfloat16), "dy": (loud * dy * (SEQUENCES * TOKENS) ** -0.5).astype(jnp.bfloat16)}
    for key, name in zip(kw, NAMES, strict=True):
        w = jax.random.normal(key, SHAPES[name], jnp.float32) * SHAPES[name][1] ** -0.5
        drawn[name] = (w * {"w_gate": 1.0, "w_up": bump(kh, FF, 4.0), "w_down": layers}[name]).astype(jnp.bfloat16)
    for key, name in zip(km, NAMES, strict=True):
        drawn[f"m_{name}"] = 0.1 * jax.random.normal(key, SHAPES[name], jnp.float32)
    for key, name in zip(kv, NAMES, strict=True):
        drawn[f"v_{name}"] = jax.random.uniform(key, SHAPES[name], jnp.float32, 0.005, 0.015)
    return drawn


def matmul(a, w):
    return jnp.dot(a, w, preferred_element_type=jnp.float32).astype(jnp.bfloat16)


def normed(h):
    wide = h.astype(jnp.float32)
    scale = lax.rsqrt(jnp.mean(wide**2, -1, keepdims=True) + 1e-6)
    return (wide * scale).astype(jnp.bfloat16)


def layer(h, w):
    a = normed(h)
    gate = jnp.dot(a, w["w_gate"], preferred_element_type=jnp.float32)
    up = jnp.dot(a, w["w_up"], preferred_element_type=jnp.float32)
    return h + matmul((jax.nn.silu(gate) * up).astype(jnp.bfloat16), w["w_down"])


def adamw(w, m, v, g):
    m = 0.9 * m + 0.1 * g
    v = 0.95 * v + 0.05 * g * g
    step = m * lax.rsqrt(v + 1e-8) + 0.1 * w
    return (w - 0.02 * step).astype(jnp.bfloat16), m, v


def clipped(gradients, sum_of_squares, count):
    factor = jnp.minimum(1.0, 0.5 * lax.rsqrt(sum_of_squares / count + 1e-30))
    return [g * factor for g in gradients]


def stack(weights, h):
    return lax.scan(lambda h, w: (layer(h, w), None), h, weights)[0]


def reference(x, dy, w_gate, w_up, w_down, m_w_gate, m_w_up, m_w_down, v_w_gate, v_w_up, v_w_down):
    weights = dict(zip(NAMES, (w_gate, w_up, w_down), strict=True))

    def take(so_far, sequence):
        h, by_y = sequence
        _, back = jax.vjp(lambda w: stack(w, h), weights)
        return jax.tree.map(lambda total, term: total + term.astype(jnp.float32), so_far, back(by_y)[0]), None

    none_yet = {name: jnp.zeros(w.shape, jnp.float32) for name, w in weights.items()}
    by_weights, _ = lax.scan(take, none_yet, (x, dy))
    gradients = [by_weights[name].astype(jnp.bfloat16).astype(jnp.float32) for name in NAMES]
    gradients = clipped(gradients, sum(jnp.sum(g * g) for g in gradients), sum(g.size for g in gradients))
    new = [
        adamw(w.astype(jnp.float32), m, v, g)
        for w, m, v, g in zip((w_gate, w_up, w_down), (m_w_gate, m_w_up, m_w_down), (v_w_gate, v_w_up, v_w_down), gradients, strict=True)
    ]
    return tuple(one[which] for which in range(3) for one in new)
```

```python
import functools

import jax
import jax.numpy as jnp
from jax import lax
from jax.experimental import pallas as pl
from jax.experimental.pallas import tpu as pltpu
from jax.sharding import PartitionSpec as P

BF16, F32 = jnp.bfloat16, jnp.float32
VMEM_LIMIT = 62 * 2**20


def dot(a, b):
    return jnp.dot(a, b, preferred_element_type=F32)


def dot_t(a, b):
    return lax.dot_general(a, b, (((1,), (1,)), ((), ())), preferred_element_type=F32)


def t_dot(a, b):
    return lax.dot_general(a, b, (((0,), (0,)), ((), ())), preferred_element_type=F32)


def inverse_rms(wide):
    return lax.rsqrt(jnp.mean(wide * wide, -1, keepdims=True) + 1e-6)


def params(dims):
    return pltpu.CompilerParams(dimension_semantics=("arbitrary",) * dims, vmem_limit_bytes=VMEM_LIMIT)


def cost(units):
    return pl.CostEstimate(flops=int(units * 14.5e9), bytes_accessed=50_000_000, transcendentals=0)


def forward_kernel(nc, nt, x_ref, wg_ref, wu_ref, wd_ref, gate_ref, up_ref, a_out, h_out, a1_out, a_s, hid_s):
    c, t = pl.program_id(0), pl.program_id(1)
    tm = x_ref.shape[0]
    fc = wg_ref.shape[1]
    rows = pl.ds(pl.multiple_of(t * tm, tm), tm)

    @pl.when(c == 0)
    def _():
        wide = x_ref[...].astype(F32)
        a = (wide * inverse_rms(wide)).astype(BF16)
        a_s[rows, :] = a
        a_out[...] = a

    for k in range(nc):
        @pl.when(c == k)
        def _(k=k):
            a = a_s[rows, :]
            gate, up = dot(a, wg_ref[...]), dot(a, wu_ref[...])
            gate_ref[...] = gate
            up_ref[...] = up
            hid_s[rows, k * fc : (k + 1) * fc] = (gate * jax.nn.sigmoid(gate) * up).astype(BF16)

    @pl.when(c == nc)
    def _():
        h = x_ref[...] + dot(hid_s[rows, :], wd_ref[...]).astype(BF16)
        h_out[...] = h
        wide = h.astype(F32)
        a1_out[...] = (wide * inverse_rms(wide)).astype(BF16)


def forward(x, wg, wu, wd, tm=512, fc=768):
    tokens, d = x.shape
    ff = wg.shape[1]
    nc, nt = ff // fc, tokens // tm
    col = lambda c, t: (0, jnp.minimum(c, nc - 1))
    tile = lambda c, t: (jnp.where(c == nc, nt - 1, t), jnp.minimum(c, nc - 1))
    first = lambda c, t: (jnp.where(c == 0, t, nt - 1), 0)
    last = lambda c, t: (jnp.where(c == nc, t, 0), 0)
    return pl.pallas_call(
        functools.partial(forward_kernel, nc, nt),
        grid=(nc + 1, nt),
        in_specs=[
            pl.BlockSpec((tm, d), lambda c, t: (jnp.where((c == 0) | (c == nc), t, nt - 1), 0)),
            pl.BlockSpec((d, fc), col),
            pl.BlockSpec((d, fc), col),
            pl.BlockSpec((ff, d), lambda c, t: (0, 0), pipeline_mode=pl.Buffered(1)),
        ],
        out_specs=[pl.BlockSpec((tm, fc), tile), pl.BlockSpec((tm, fc), tile), pl.BlockSpec((tm, d), first), pl.BlockSpec((tm, d), last), pl.BlockSpec((tm, d), last)],
        out_shape=[jax.ShapeDtypeStruct((tokens, ff), F32)] * 2 + [jax.ShapeDtypeStruct((tokens, d), BF16)] * 3,
        scratch_shapes=[pltpu.VMEM((tokens, d), BF16), pltpu.VMEM((tokens, ff), BF16)],
        compiler_params=params(2),
        cost_estimate=cost(3),
        name="forward0",
    )(x, wg, wu, wd)


def hidden_grads(gate, up, dhid):
    dhid = dhid.astype(BF16).astype(F32)
    sig = jax.nn.sigmoid(gate)
    silu = gate * sig
    hid = (silu * up).astype(BF16)
    dup = (dhid * silu).astype(BF16)
    dgate = (dhid * up * (sig * (1 + gate * (1 - sig)))).astype(BF16)
    return hid, dgate, dup


def layer1_kernel(nt, a_ref, dy_ref, wg_ref, wu_ref, wd_ref, dwg_ref, dwu_ref, dwd_ref, dgate_ref, dup_ref, acg, acu, acd):
    t = pl.program_id(1)

    @pl.when(t == 0)
    def _():
        for acc in (acg, acu, acd):
            acc[...] = jnp.zeros_like(acc)

    a, dy = a_ref[...], dy_ref[...]
    hid, dgate, dup = hidden_grads(dot(a, wg_ref[...]), dot(a, wu_ref[...]), dot_t(dy, wd_ref[...]))
    dgate_ref[...] = dgate
    dup_ref[...] = dup
    acd[...] += t_dot(hid, dy)
    acg[...] += t_dot(a, dgate)
    acu[...] += t_dot(a, dup)

    @pl.when(t == nt - 1)
    def _():
        for out, acc in ((dwg_ref, acg), (dwu_ref, acu), (dwd_ref, acd)):
            out[...] = acc[...].astype(BF16)


def layer1(a, dy, wg, wu, wd, tm=1024, fc=768):
    tokens, d = a.shape
    ff = wg.shape[1]
    nc, nt = ff // fc, tokens // tm
    row, col, chunk, tile = (lambda c, t: (t, 0)), (lambda c, t: (0, c)), (lambda c, t: (c, 0)), (lambda c, t: (t, c))
    return pl.pallas_call(
        functools.partial(layer1_kernel, nt),
        grid=(nc, nt),
        in_specs=[pl.BlockSpec((tm, d), row)] * 2 + [pl.BlockSpec((d, fc), col)] * 2 + [pl.BlockSpec((fc, d), chunk)],
        out_specs=[pl.BlockSpec((d, fc), col)] * 2 + [pl.BlockSpec((fc, d), chunk)] + [pl.BlockSpec((tm, fc), tile)] * 2,
        out_shape=[jax.ShapeDtypeStruct((d, ff), BF16)] * 2 + [jax.ShapeDtypeStruct((ff, d), BF16)] + [jax.ShapeDtypeStruct((tokens, ff), BF16)] * 2,
        scratch_shapes=[pltpu.VMEM((d, fc), F32), pltpu.VMEM((d, fc), F32), pltpu.VMEM((fc, d), F32)],
        compiler_params=params(2),
        cost_estimate=cost(6),
        name="layer1",
    )(a, dy, wg, wu, wd)


def input_grad_kernel(dgate_ref, dup_ref, h_ref, dy_ref, wg_ref, wu_ref, out_ref):
    dn = (dot_t(dgate_ref[...], wg_ref[...]) + dot_t(dup_ref[...], wu_ref[...])).astype(BF16).astype(F32)
    wide = h_ref[...].astype(F32)
    scale = inverse_rms(wide)
    along = jnp.sum(dn * wide, -1, keepdims=True) * (scale * scale * scale) * (1.0 / wide.shape[-1])
    out_ref[...] = dy_ref[...] + (dn * scale - wide * along).astype(BF16)


def input_grad(dgate, dup, h, dy, wg, wu, tm=512):
    tokens, d = h.shape
    ff = wg.shape[1]
    row, whole = (lambda t: (t, 0)), (lambda t: (0, 0))
    return pl.pallas_call(
        input_grad_kernel,
        grid=(tokens // tm,),
        in_specs=[pl.BlockSpec((tm, ff), row)] * 2 + [pl.BlockSpec((tm, d), row)] * 2 + [pl.BlockSpec((d, ff), whole, pipeline_mode=pl.Buffered(1))] * 2,
        out_specs=pl.BlockSpec((tm, d), row),
        out_shape=jax.ShapeDtypeStruct((tokens, d), BF16),
        compiler_params=params(1),
        cost_estimate=cost(2),
        name="input_grad",
    )(dgate, dup, h, dy, wg, wu)


def layer0_kernel(nt, a_ref, dy_ref, gate_ref, up_ref, wd_ref, dwg_ref, dwu_ref, dwd_ref, acg, acu, acd):
    t = pl.program_id(1)

    @pl.when(t == 0)
    def _():
        for acc in (acg, acu, acd):
            acc[...] = jnp.zeros_like(acc)

    a, dy = a_ref[...], dy_ref[...]
    hid, dgate, dup = hidden_grads(gate_ref[...], up_ref[...], dot_t(dy, wd_ref[...]))
    acd[...] += t_dot(hid, dy)
    acg[...] += t_dot(a, dgate)
    acu[...] += t_dot(a, dup)

    @pl.when(t == nt - 1)
    def _():
        for out, acc in ((dwg_ref, acg), (dwu_ref, acu), (dwd_ref, acd)):
            out[...] = acc[...].astype(BF16)


def layer0(a, dy, gate, up, wd, tm=1024, fc=768):
    tokens, d = a.shape
    ff = wd.shape[0]
    nc, nt = ff // fc, tokens // tm
    row, col, chunk, tile = (lambda c, t: (t, 0)), (lambda c, t: (0, c)), (lambda c, t: (c, 0)), (lambda c, t: (t, c))
    return pl.pallas_call(
        functools.partial(layer0_kernel, nt),
        grid=(nc, nt),
        in_specs=[pl.BlockSpec((tm, d), row)] * 2 + [pl.BlockSpec((tm, fc), tile)] * 2 + [pl.BlockSpec((fc, d), chunk)],
        out_specs=[pl.BlockSpec((d, fc), col)] * 2 + [pl.BlockSpec((fc, d), chunk)],
        out_shape=[jax.ShapeDtypeStruct((d, ff), BF16)] * 2 + [jax.ShapeDtypeStruct((ff, d), BF16)],
        scratch_shapes=[pltpu.VMEM((d, fc), F32), pltpu.VMEM((d, fc), F32), pltpu.VMEM((fc, d), F32)],
        compiler_params=params(2),
        cost_estimate=cost(4),
        name="layer0",
    )(a, dy, gate, up, wd)


def adamw(w, m, v, g):
    m = 0.9 * m + 0.1 * g
    v = 0.95 * v + 0.05 * g * g
    step = m * lax.rsqrt(v + 1e-8) + 0.1 * w
    return (w - 0.02 * step).astype(BF16), m, v


def clipped(gradients, sum_of_squares, count):
    factor = jnp.minimum(1.0, 0.5 * lax.rsqrt(sum_of_squares / count + 1e-30))
    return [g * factor for g in gradients]


def solution(mesh):
    reps = mesh.shape["rep"]

    def fetched(block):
        share = block.shape[0] // reps
        mine = lax.dynamic_slice_in_dim(block, lax.axis_index("rep") * share, share, 0)
        return lax.all_gather(mine, ("dp", "rep"), axis=0, tiled=True)

    def step(x, dy, *arrays):
        weights, m, v = (arrays[i : i + 3] for i in (0, 3, 6))
        layers = weights[0].shape[0]
        w = [[fetched(one[number]) for one in weights] for number in range(layers)]
        gate, up, a0, h1, a1 = forward(x[0], *w[0])
        dwg1, dwu1, dwd1, dgate, dup = layer1(a1, dy[0], *w[1])
        scatter = lambda g: lax.psum_scatter(g, "dp", scatter_dimension=0, tiled=True)
        mine1 = [scatter(g) for g in (dwg1, dwu1, dwd1)]
        dy0 = input_grad(dgate, dup, h1, dy[0], w[1][0], w[1][1])
        mine0 = [scatter(g) for g in layer0(a0, dy0, gate, up, w[0][2])]
        gradients = [jnp.stack(pair).astype(F32) for pair in zip(mine0, mine1)]
        squares = lax.psum(sum(jnp.sum(g * g) for g in gradients), "dp")
        gradients = clipped(gradients, squares, lax.psum(1, "dp") * sum(g.size for g in gradients))
        new = [adamw(w.astype(F32), m, v, g) for w, m, v, g in zip(weights, m, v, gradients, strict=True)]
        return tuple(one[which] for which in range(3) for one in new)

    states, cut = P(("rep", "dp"), None, None), P(None, "dp", None)
    return jax.shard_map(
        step,
        mesh=mesh,
        in_specs=(states, states) + (cut,) * 9,
        out_specs=(P("rep", "dp", None),) * 9,
        check_vma=False,
    )
```

```python
import functools

import jax
import jax.numpy as jnp
from jax import lax
from jax.experimental import pallas as pl
from jax.experimental.pallas import tpu as pltpu
from jax.sharding import PartitionSpec as P

BF16, F32 = jnp.bfloat16, jnp.float32
VMEM_LIMIT = 63 * 2**20
CHIPS = 4
VMEM = pltpu.VMEM
DMA = pltpu.SemaphoreType.DMA


def dot(a, b):
    return jnp.dot(a, b, preferred_element_type=F32)


def dot_t(a, b):
    return lax.dot_general(a, b, (((1,), (1,)), ((), ())), preferred_element_type=F32)


def t_dot(a, b):
    return lax.dot_general(a, b, (((0,), (0,)), ((), ())), preferred_element_type=F32)


def inverse_rms(wide):
    return lax.rsqrt(jnp.mean(wide * wide, -1, keepdims=True) + 1e-6)


def params(dims, **more):
    return pltpu.CompilerParams(dimension_semantics=("arbitrary",) * dims, vmem_limit_bytes=VMEM_LIMIT, **more)


def cost(units):
    return pl.CostEstimate(flops=int(units * 14.5e9), bytes_accessed=50_000_000, transcendentals=0)


def resident(shape):
    return pl.BlockSpec(shape, lambda *_: (0,) * len(shape), pipeline_mode=pl.Buffered(1))


class Place:
    def __init__(self):
        self.me = lax.axis_index("dp")
        self.z, self.core = self.me // 2, self.me % 2
        self.partner = self.me + 1 - 2 * self.core

    def greet(self):
        barrier = pltpu.get_barrier_semaphore()
        signal = lambda to: pl.semaphore_signal(barrier, inc=1, device_id={"dp": to}, device_id_type=pl.DeviceIdType.MESH)
        signal(self.partner)
        pl.when(self.z > 0)(lambda: signal(self.me - 2))
        pl.when(self.z < CHIPS - 1)(lambda: signal(self.me + 2))

    def greeted(self):
        peers = 1 + (self.z + CHIPS - 1) // CHIPS + (2 * CHIPS - 2 - self.z) // CHIPS
        pl.semaphore_wait(pltpu.get_barrier_semaphore(), peers)


def remote(src, dst, send_sem, recv_sem, to):
    return pltpu.make_async_remote_copy(src, dst, send_sem, recv_sem, device_id={"dp": to}, device_id_type=pl.DeviceIdType.MESH)


class Sum:
    def __init__(self, place, own, theirs, arriving, leaving, out, sems):
        self.place, self.own, self.theirs, self.arriving, self.leaving, self.out = place, own, theirs, arriving, leaving, out
        self.half_sems, self.arrive_sems, self.leave_sems = sems
        self.n = own.shape[1]

    @staticmethod
    def scratch(n, share, d):
        return [
            VMEM((n, CHIPS, share, d), BF16),
            VMEM((2, 3, n, share, d), BF16),
            VMEM((2, 3, n, share, d), BF16),
            DMA((2,)),
            DMA((2, 3, n)),
            DMA((2, 3, n)),
        ]

    @staticmethod
    def on(place, own, out, scratch):
        theirs, arriving, leaving, *sems = scratch
        return Sum(place, own, theirs, arriving, leaving, out, sems)

    def halves(self):
        p = self.place
        return remote(self.own.at[1 - p.core], self.theirs, self.half_sems.at[0], self.half_sems.at[1], p.partner)

    def copy(self, way, k, m):
        to = self.place.me + (2, -2)[way]
        return remote(self.leaving.at[way, k, m], self.arriving.at[way, k, m], self.leave_sems.at[way, k, m], self.arrive_sems.at[way, k, m], to)

    def mine(self, m, chip):
        return self.own[self.place.core, m, chip].astype(F32) + self.theirs[m, chip].astype(F32)

    def send(self, k, m):
        z = self.place.z
        for way, behind, chip in ((0, z, 3 + z - k), (1, 3 - z, z - 3 + k)):

            @pl.when((behind <= k) & (behind < 3))
            def _(way=way, behind=behind, chip=chip):
                before = (k + 2) % 3

                @pl.when(behind > 0)
                def _():
                    self.copy(way, before, m).wait_recv()

                total = self.mine(m, chip) + jnp.where(behind > 0, self.arriving[way, before, m].astype(F32), 0.0)
                self.leaving[way, k, m] = total.astype(BF16)
                self.copy(way, k, m).start()

    def finish(self, m):
        z = self.place.z
        pl.when(z > 0)(lambda: self.copy(0, 2, m).wait_recv())
        pl.when(z < 3)(lambda: self.copy(1, 2, m).wait_recv())
        total = self.mine(m, z)
        for way, there in ((0, z > 0), (1, z < 3)):
            total += jnp.where(there, self.arriving[way, 2, m].astype(F32), 0.0)
        self.out[m] = total.astype(BF16)

    def tick(self, i):
        k, m = i // self.n, i % self.n
        pl.when(k < 3)(lambda: self.send(k, m))
        pl.when(k == 3)(lambda: self.finish(m))

    def drain(self):
        z = self.place.z
        for way, behind in ((0, z), (1, 3 - z)):
            for k in range(3):

                @pl.when((behind <= k) & (behind < 3))
                def _(way=way, k=k):
                    for m in range(self.n):
                        self.copy(way, k, m).wait_send()


def keep(own, m, acc):
    share = acc.shape[0] // (2 * CHIPS)
    for chip in range(CHIPS):
        for core in range(2):
            at = (2 * chip + core) * share
            own[core, m, chip] = acc[at : at + share, :].astype(BF16)


def forward_kernel(nc, nt, x_ref, wg_ref, wu_ref, wd_ref, gate_ref, up_ref, hid_out, a_out, h_out, a1_out, a_s, hid_s):
    c, t = pl.program_id(0), pl.program_id(1)
    tm = x_ref.shape[0]
    fc = wg_ref.shape[1]
    rows = pl.ds(pl.multiple_of(t * tm, tm), tm)

    @pl.when(c == 0)
    def _():
        wide = x_ref[...].astype(F32)
        a = (wide * inverse_rms(wide)).astype(BF16)
        a_s[rows, :] = a
        a_out[...] = a

    for k in range(nc):
        @pl.when(c == k)
        def _(k=k):
            a = a_s[rows, :]
            gate, up = dot(a, wg_ref[...]), dot(a, wu_ref[...])
            gate_ref[...] = gate
            up_ref[...] = up
            hid = (gate * jax.nn.sigmoid(gate) * up).astype(BF16)
            hid_s[rows, k * fc : (k + 1) * fc] = hid
            hid_out[...] = hid

    @pl.when(c == nc)
    def _():
        h = x_ref[...] + dot(hid_s[rows, :], wd_ref[...]).astype(BF16)
        h_out[...] = h
        wide = h.astype(F32)
        a1_out[...] = (wide * inverse_rms(wide)).astype(BF16)


def forward(x, wg, wu, wd, tm=512, fc=768):
    tokens, d = x.shape
    ff = wg.shape[1]
    nc, nt = ff // fc, tokens // tm
    col = lambda c, t: (0, jnp.minimum(c, nc - 1))
    tile = lambda c, t: (jnp.where(c == nc, nt - 1, t), jnp.minimum(c, nc - 1))
    first = lambda c, t: (jnp.where(c == 0, t, nt - 1), 0)
    last = lambda c, t: (jnp.where(c == nc, t, 0), 0)
    return pl.pallas_call(
        functools.partial(forward_kernel, nc, nt),
        grid=(nc + 1, nt),
        in_specs=[
            pl.BlockSpec((tm, d), lambda c, t: (jnp.where((c == 0) | (c == nc), t, nt - 1), 0)),
            pl.BlockSpec((d, fc), col),
            pl.BlockSpec((d, fc), col),
            resident((ff, d)),
        ],
        out_specs=[pl.BlockSpec((tm, fc), tile)] * 3 + [pl.BlockSpec((tm, d), first), pl.BlockSpec((tm, d), last), pl.BlockSpec((tm, d), last)],
        out_shape=[jax.ShapeDtypeStruct((tokens, ff), F32)] * 2
        + [jax.ShapeDtypeStruct((tokens, ff), BF16)]
        + [jax.ShapeDtypeStruct((tokens, d), BF16)] * 3,
        scratch_shapes=[VMEM((tokens, d), BF16), VMEM((tokens, ff), BF16)],
        compiler_params=params(2),
        cost_estimate=cost(3),
        name="forward0",
    )(x, wg, wu, wd)


def hidden_grads(gate, up, dhid):
    dhid = dhid.astype(BF16).astype(F32)
    sig = jax.nn.sigmoid(gate)
    silu = gate * sig
    hid = (silu * up).astype(BF16)
    dup = (dhid * silu).astype(BF16)
    dgate = (dhid * up * (sig * (1 + gate * (1 - sig)))).astype(BF16)
    return hid, dgate, dup


def layer1_kernel(nc, nt, a_ref, dy_ref, wg_ref, wu_ref, wd_ref, dgate_ref, dup_ref, own_ref, sum_ref, acg, acu, acd, *scratch):
    c, t = pl.program_id(0), pl.program_id(1)
    place = Place()
    half = len(scratch) // 2
    sums = [Sum.on(place, own_ref, sum_ref.at[g], scratch[g * half : (g + 1) * half]) for g in range(2)]

    def tick(j):
        for g, one in enumerate(sums):
            @pl.when(c == g + 1)
            def _(one=one):
                if j == 0:
                    pl.when(t == 0)(lambda: one.halves().wait())
                one.tick(3 * t + j)

    @pl.when((c == 0) & (t == 0))
    def _():
        place.greet()

    @pl.when((c == 0) & (t == 1))
    def _():
        place.greeted()

    @pl.when(t == 0)
    def _():
        for acc in (acg, acu, acd):
            acc[...] = jnp.zeros_like(acc)

    a, dy = a_ref[...], dy_ref[...]
    gate, up = dot(a, wg_ref[...]), dot(a, wu_ref[...])
    tick(0)
    hid, dgate, dup = hidden_grads(gate, up, dot_t(dy, wd_ref[...]))
    dgate_ref[...] = dgate
    dup_ref[...] = dup
    tick(1)
    acd[...] += t_dot(hid, dy)
    acg[...] += t_dot(a, dgate)
    tick(2)
    acu[...] += t_dot(a, dup)

    @pl.when(t == nt - 1)
    def _():
        for m, acc in enumerate((acg, acu, acd)):
            keep(own_ref, m, acc)
        for g, one in enumerate(sums):
            @pl.when(c == g)
            def _(g=g, one=one):
                one.halves().start()

            pl.when(c == g + 1)(one.drain)


def layer1(a, dy, wg, wu, wd, tm=1024, fc=768):
    tokens, d = a.shape
    ff = wg.shape[1]
    nc, nt = ff // fc, tokens // tm
    share = d // (2 * CHIPS)
    row, col, chunk, tile = (lambda c, t: (t, 0)), (lambda c, t: (0, c)), (lambda c, t: (c, 0)), (lambda c, t: (t, c))
    own, out = (2, 3, CHIPS, share, d), (2, 3, share, d)
    return pl.pallas_call(
        functools.partial(layer1_kernel, nc, nt),
        grid=(nc, nt),
        in_specs=[pl.BlockSpec((tm, d), row)] * 2 + [pl.BlockSpec((d, fc), col)] * 2 + [pl.BlockSpec((fc, d), chunk)],
        out_specs=[pl.BlockSpec((tm, fc), tile)] * 2 + [resident(own), resident(out)],
        out_shape=[jax.ShapeDtypeStruct((tokens, ff), BF16)] * 2 + [jax.ShapeDtypeStruct(own, BF16), jax.ShapeDtypeStruct(out, BF16)],
        scratch_shapes=[VMEM((d, fc), F32), VMEM((d, fc), F32), VMEM((fc, d), F32)] + Sum.scratch(3, share, d) * 2,
        compiler_params=params(2, collective_id=1, has_side_effects=True),
        cost_estimate=cost(6),
        name="layer1",
    )(a, dy, wg, wu, wd)


def between_kernel(nt, dgate_ref, dup_ref, h_ref, dy_ref, hid_ref, wg_ref, wu_ref, own_in, out_ref, own_ref, sum_ref, acd, *scratch):
    t = pl.program_id(0)
    place = Place()
    one = Sum.on(place, own_in, sum_ref, scratch)

    @pl.when(t == 0)
    def _():
        place.greet()
        acd[...] = jnp.zeros_like(acd)

    @pl.when(t == 1)
    def _():
        place.greeted()
        one.halves().start()

    def tick(j):
        @pl.when(t >= 2)
        def _():
            if j == 0:
                pl.when(t == 2)(lambda: one.halves().wait())
            one.tick(2 * (t - 2) + j)

    tick(0)
    dn = (dot_t(dgate_ref[...], wg_ref[...]) + dot_t(dup_ref[...], wu_ref[...])).astype(BF16).astype(F32)
    wide = h_ref[...].astype(F32)
    scale = inverse_rms(wide)
    along = jnp.sum(dn * wide, -1, keepdims=True) * (scale * scale * scale) * (1.0 / wide.shape[-1])
    dy = dy_ref[...] + (dn * scale - wide * along).astype(BF16)
    out_ref[...] = dy
    tick(1)
    acd[...] += t_dot(hid_ref[...], dy)

    @pl.when(t == nt - 1)
    def _():
        one.drain()
        rows = acd.shape[0] // 3
        for c in range(3):
            keep(own_ref, c, acd[c * rows : (c + 1) * rows, :])


def between(dgate, dup, h, dy, hid, wg, wu, own, tm=512):
    tokens, d = h.shape
    ff = wg.shape[1]
    share = d // (2 * CHIPS)
    nt = tokens // tm
    assert nt == 8
    row = lambda t: (t, 0)
    out = (3, share, d)
    return pl.pallas_call(
        functools.partial(between_kernel, nt),
        grid=(nt,),
        in_specs=[pl.BlockSpec((tm, ff), row)] * 2 + [pl.BlockSpec((tm, d), row)] * 2 + [pl.BlockSpec((tm, ff), row)] + [resident((d, ff))] * 2 + [resident(own.shape)],
        out_specs=[pl.BlockSpec((tm, d), row), resident(own.shape), resident(out)],
        out_shape=[jax.ShapeDtypeStruct((tokens, d), BF16), jax.ShapeDtypeStruct(own.shape, BF16), jax.ShapeDtypeStruct(out, BF16)],
        scratch_shapes=[VMEM((ff, d), F32)] + Sum.scratch(3, share, d),
        compiler_params=params(1, collective_id=2, has_side_effects=True),
        cost_estimate=cost(3),
        name="between",
    )(dgate, dup, h, dy, hid, wg, wu, own)


def layer0_kernel(nt, a_ref, dy_ref, gate_ref, up_ref, wd_ref, own_in, own_ref, sum0_ref, sum1_ref, acg, acu, own1, *scratch):
    c, t = pl.program_id(0), pl.program_id(1)
    place = Place()
    half = len(scratch) // 2
    first = Sum.on(place, own_in, sum0_ref, scratch[:half])
    second = Sum.on(place, own1, sum1_ref, scratch[half:])
    step = c * nt + t

    @pl.when(step == 0)
    def _():
        place.greet()

    @pl.when(step == 1)
    def _():
        place.greeted()
        first.halves().start()

    @pl.when(t == 0)
    def _():
        for acc in (acg, acu):
            acc[...] = jnp.zeros_like(acc)

    @pl.when((step >= 2) & (step < 14))
    def _():
        pl.when(step == 2)(lambda: first.halves().wait())
        first.tick(step - 2)

    @pl.when((step >= 14) & (step < 22))
    def _():
        pl.when(step == 14)(lambda: second.halves().wait())
        second.tick(step - 14)

    a, dy = a_ref[...], dy_ref[...]
    _, dgate, dup = hidden_grads(gate_ref[...], up_ref[...], dot_t(dy, wd_ref[...]))
    acg[...] += t_dot(a, dgate)
    acu[...] += t_dot(a, dup)

    @pl.when(t == nt - 1)
    def _():
        for m, acc in enumerate((acg, acu)):
            pl.when(c == 0)(lambda m=m, acc=acc: keep(own1, m, acc))
            pl.when(c == 1)(lambda m=m, acc=acc: keep(own_ref, m, acc))
            pl.when(c == 2)(lambda m=m, acc=acc: keep(own_ref, 2 + m, acc))
        pl.when(c == 0)(lambda: second.halves().start())

        @pl.when(c == 2)
        def _():
            first.drain()
            second.drain()


def layer0(a, dy, gate, up, wd, own, tm=512, fc=768):
    tokens, d = a.shape
    ff = wd.shape[0]
    nc, nt = ff // fc, tokens // tm
    share = d // (2 * CHIPS)
    row, chunk, tile = (lambda c, t: (t, 0)), (lambda c, t: (c, 0)), (lambda c, t: (t, c))
    rest, out0, out1 = (2, 4, CHIPS, share, d), (3, share, d), (2, share, d)
    return pl.pallas_call(
        functools.partial(layer0_kernel, nt),
        grid=(nc, nt),
        in_specs=[pl.BlockSpec((tm, d), row)] * 2 + [pl.BlockSpec((tm, fc), tile)] * 2 + [pl.BlockSpec((fc, d), chunk), resident(own.shape)],
        out_specs=[resident(rest), resident(out0), resident(out1)],
        out_shape=[jax.ShapeDtypeStruct(rest, BF16), jax.ShapeDtypeStruct(out0, BF16), jax.ShapeDtypeStruct(out1, BF16)],
        scratch_shapes=[VMEM((d, fc), F32), VMEM((d, fc), F32), VMEM((2, 2, CHIPS, share, d), BF16)] + Sum.scratch(3, share, d) + Sum.scratch(2, share, d),
        compiler_params=params(2, collective_id=3, has_side_effects=True),
        cost_estimate=cost(3),
        name="layer0",
    )(a, dy, gate, up, wd, own)


def rest_kernel(own_in, sum_ref, *scratch):
    place = Place()
    one = Sum.on(place, own_in, sum_ref, scratch)
    place.greet()
    place.greeted()
    one.halves().start()
    one.halves().wait()

    @pl.loop(0, 4 * one.n)
    def _(i):
        one.tick(i)

    one.drain()


def rest(own):
    _, n, _, share, d = own.shape
    return pl.pallas_call(
        rest_kernel,
        in_specs=[pl.BlockSpec(memory_space=VMEM)],
        out_specs=pl.BlockSpec(memory_space=VMEM),
        out_shape=jax.ShapeDtypeStruct((n, share, d), BF16),
        scratch_shapes=Sum.scratch(n, share, d),
        compiler_params=pltpu.CompilerParams(vmem_limit_bytes=VMEM_LIMIT, collective_id=4, has_side_effects=True),
        cost_estimate=cost(3),
        name="rest",
    )(own)


def adamw(w, m, v, g):
    m = 0.9 * m + 0.1 * g
    v = 0.95 * v + 0.05 * g * g
    step = m * lax.rsqrt(v + 1e-8) + 0.1 * w
    return (w - 0.02 * step).astype(BF16), m, v


def clipped(gradients, sum_of_squares, count):
    factor = jnp.minimum(1.0, 0.5 * lax.rsqrt(sum_of_squares / count + 1e-30))
    return [g * factor for g in gradients]


def solution(mesh):
    n = mesh.shape["dp"]

    def whole(wg, wu, wd):
        share = wg.shape[0]
        columns = lambda w: lax.all_gather(w.reshape(share, n, 3, share).transpose(0, 2, 1, 3).reshape(share, -1), "dp", axis=0, tiled=True)
        rows = lax.all_gather(wd.reshape(3, share, -1), "dp", axis=1, tiled=True).reshape(-1, wd.shape[1])
        return columns(wg), columns(wu), rows

    def natural(chunks):
        share = chunks.shape[1]
        return chunks.reshape(3, share, n, share).transpose(1, 2, 0, 3).reshape(share, -1)

    def step(x, dy, *arrays):
        weights, m, v = (arrays[i : i + 3] for i in (0, 3, 6))
        w0, w1 = (whole(*(one[number] for one in weights)) for number in range(2))
        gate, up, hid, a0, h1, a1 = forward(x[0], *w0)
        dgate, dup, own, first = layer1(a1, dy[0], *w1)
        dy0, own, second = between(dgate, dup, h1, dy[0], hid, w1[0], w1[1], own)
        own, down0, third = layer0(a0, dy0, gate, up, w0[2], own)
        last = rest(own)
        one = jnp.concatenate([first, second[None]])
        mine1 = [natural(one[:, 0]), natural(one[:, 1]), one[:, 2].reshape(-1, one.shape[-1])]
        pair = jnp.concatenate([third[None], last.reshape(2, 2, *last.shape[1:])])
        mine0 = [natural(pair[:, 0]), natural(pair[:, 1]), down0.reshape(-1, down0.shape[-1])]
        gradients = [jnp.stack(both).astype(F32) for both in zip(mine0, mine1)]
        squares = lax.psum(sum(jnp.sum(g * g) for g in gradients), "dp")
        gradients = clipped(gradients, squares, n * sum(g.size for g in gradients))
        new = [adamw(w.astype(F32), m, v, g) for w, m, v, g in zip(weights, m, v, gradients, strict=True)]
        return tuple(one[which] for which in range(3) for one in new)

    states, cut = P(("rep", "dp"), None, None), P(None, "dp", None)
    return jax.shard_map(
        step,
        mesh=mesh,
        in_specs=(states, states) + (cut,) * 9,
        out_specs=(P("rep", "dp", None),) * 9,
        check_vma=False,
    )
```
